32 devices in a mesh: group: 2 (over x), grid: 8 (over z, y), var: 2 (over core).
Axes of the slice: x: 2, y: 2, z: 4, core: 2. Of those that a mesh axis runs over, the one named last changes fastest.
Arguments:
- tokens: bfloat16 [96, 96, 3, 512], P('group', 'grid'), parts along dimension 0, may hold values from -6 to 6
- key_mask: int32 [96, 96], P('group', 'grid'), parts along dimension 0, may hold values 0 or 1
- w_qkv: bfloat16 [3, 512, 512], P(None, None, 'var'), may hold values from -16 to 16
- w_proj: bfloat16 [512, 512], P('var'), may hold values from -0.25 to 0.25
- w_up: bfloat16 [512, 2048], P(None, 'var'), may hold values from -0.25 to 0.25
- w_down: bfloat16 [2048, 512], P('var'), may hold values from -0.125 to 0.125
- level_query: bfloat16 [13, 512], replicated, may hold values from -1200 to 1200
- w_dec_q: bfloat16 [512, 512], P(None, 'var'), may hold values from -0.25 to 0.25
- w_dec_kv: bfloat16 [2, 512, 512], P(None, None, 'var'), may hold values from -0.25 to 0.25
- w_dec_o: bfloat16 [512, 512], P('var'), may hold values from -0.25 to 0.25
- decode_matrix: float32 [512, 64], replicated, may hold values from -0.25 to 0.25
Outputs:
- estimated_maps: float32 [4, 26, 192, 384], P('var', 'group', 'grid'), parts along dimension 1
The draws below stay inside these ranges and needn't reach their ends.
There are 2 independent parts, one for each index of `group`. The reference program is written for one: setup_inputs(seed, part) draws one part's arguments, and reference() takes and returns one part's arrays. A program takes and returns all parts, laid end to end along the dimension named above; an argument that names none is the same for every part. Nothing has to cross between parts.
All inputs are finite; a program needn't handle non-finite values. No bound on the sum of `key_mask` on one device may be relied on, other than what follows from the above.
Results may differ from the reference program's by a relative error of at most 0.025.
Values may be sent and summed in bfloat16 or wider, within the bound.
No kernel may reach another device: no remote copies, remote signals or barrier semaphores. Data moves between devices by JAX's collectives and lax.ppermute only.
A program may use at most 128 MiB of HBM per device.

```python
import jax
import jax.numpy as jnp
from jax import lax

EMBED_WIDTH = 512
HD = 64
FF = 2048
TARGET_QUANTITY = 4
ISOBAR_NUMBER = 13
LEV = 3
SQUARE_SPAN = 4
WIN_LAT = 6
WINDOW_EASTWARD = 12
LAT = 48
LON = 96


def draw_w_qkv(key, part):
    key = jax.random.fold_in(key, 11)
    base_key = jax.random.fold_in(key, 0)
    result = jnp.clip(jax.random.normal(base_key, (3, EMBED_WIDTH, EMBED_WIDTH), jnp.float32), -6.0, 6.0) * EMBED_WIDTH ** (-0.5)
    return result.astype(jnp.bfloat16)


def draw_level_query(key, part):
    key = jax.random.fold_in(key, 23)
    base_key = jax.random.fold_in(key, 0)
    result = jnp.clip(jax.random.normal(base_key, (ISOBAR_NUMBER, EMBED_WIDTH), jnp.float32), -6.0, 6.0)
    return result.astype(jnp.bfloat16)


def touch_ends(array, rng, smallest, top_value):
    shape = array.shape
    spot = [jax.random.randint(jax.random.fold_in(rng, axis), (), 0, shape[axis]) for axis in range(len(shape))]
    array = array.at[tuple(spot)].set(smallest)
    longest = shape.index(max(shape))
    spot[longest] = (spot[longest] + 1) % shape[longest]
    return array.at[tuple(spot)].set(top_value)


def shard_levels(key, shape, pieces, low, high):
    level, own = 1.0, jax.random.fold_in(key, 6)
    for dim, blocks in pieces:
        heights = jnp.exp(jax.random.uniform(jax.random.fold_in(own, dim), (blocks,), jnp.float32, low / len(pieces), high / len(pieces)))
        level = level * jnp.repeat(heights, shape[dim] // blocks).reshape([-1 if axis == dim else 1 for axis in range(len(shape))])
    return level


def normal_values(key, dims, scale, bound, cuts=(), dtype=jnp.bfloat16):
    level = shard_levels(key, dims, cuts, -0.22, 0.18) if cuts else 1.0
    entries = jax.random.normal(key, dims, jnp.float32) * scale * level
    return jnp.minimum(jnp.maximum(entries, -bound), bound).astype(dtype)


def setup_inputs(seed: int = 0, part: int = 0) -> dict:
    streams_of = jax.random.split(jax.random.key(seed), 12)
    part_splits = jax.random.split(jax.random.fold_in(streams_of[11], part), 12)
    return {
        "tokens": normal_values(part_splits[0], (LAT, LON, LEV, EMBED_WIDTH), 1.0, 6.0, ((1, 8),)),
        "key_mask": touch_ends((jax.random.randint(part_splits[1], (LAT, LON), 0, 4) < 3).astype(jnp.int32), jax.random.fold_in(part_splits[1], 1), 0, 1),
        "w_qkv": draw_w_qkv(jax.random.fold_in(streams_of[11], 71), part),
        "w_proj": normal_values(streams_of[3], (EMBED_WIDTH, EMBED_WIDTH), EMBED_WIDTH ** -0.5, 0.25, ((0, 2),)),
        "w_up": normal_values(streams_of[4], (EMBED_WIDTH, FF), EMBED_WIDTH ** -0.5, 0.25, ((1, 2),)),
        "w_down": normal_values(streams_of[5], (FF, EMBED_WIDTH), FF ** -0.5, 0.125, ((0, 2),)),
        "level_query": draw_level_query(jax.random.fold_in(streams_of[11], 71), part),
        "w_dec_q": normal_values(streams_of[7], (EMBED_WIDTH, EMBED_WIDTH), EMBED_WIDTH ** -0.5, 0.25, ((1, 2),)),
        "w_dec_kv": normal_values(streams_of[8], (2, EMBED_WIDTH, EMBED_WIDTH), EMBED_WIDTH ** -0.5, 0.25, ((2, 2),)),
        "w_dec_o": normal_values(streams_of[9], (EMBED_WIDTH, EMBED_WIDTH), EMBED_WIDTH ** -0.5, 0.25, ((0, 2),)),
        "decode_matrix": normal_values(streams_of[10], (EMBED_WIDTH, TARGET_QUANTITY * SQUARE_SPAN * SQUARE_SPAN), EMBED_WIDTH ** -0.5, 0.25, (), jnp.float32),
    }


EPSILON = 1e-05

def layer_norm(values):
    center = values - lax.optimization_barrier(jnp.mean(values, axis=-1, keepdims=True))
    spread = lax.optimization_barrier(jnp.mean(center * center, axis=-1, keepdims=True))
    return center * lax.rsqrt(spread + EPSILON)

def window_attention(tile_tokens, key_marks, row_start, total_rows, w_qkv, w_proj):
    north_south_circles, columns, levels, features = tile_tokens.shape
    local_width = w_qkv.shape[2]
    head_count = local_width // HD
    normed = layer_norm(tile_tokens.astype(jnp.float32)).astype(jnp.bfloat16).reshape(-1, features)
    win_count = north_south_circles // WIN_LAT
    tok_count = WIN_LAT * columns * levels

    def project(which):
        result = jnp.dot(normed, w_qkv[which], preferred_element_type=jnp.float32)
        return result.astype(jnp.bfloat16).reshape(win_count, tok_count, head_count, HD)
    queries = project(0)
    key_heads = project(1)
    value_heads = project(2)
    scores = jnp.einsum('wqhd,wkhd->whqk', queries.astype(jnp.float32), key_heads.astype(jnp.float32)) * HD ** (-0.5)
    row_index = lax.broadcasted_iota(jnp.int32, (north_south_circles, columns, levels), 0).reshape(win_count, tok_count)
    region = row_index + row_start >= total_rows - WIN_LAT // 2
    open_key = jnp.broadcast_to(key_marks[:, :, None], (north_south_circles, columns, levels)).reshape(win_count, tok_count) > 0
    diagonal = lax.broadcasted_iota(jnp.int32, (tok_count, tok_count), 0) == lax.broadcasted_iota(jnp.int32, (tok_count, tok_count), 1)
    allowed = (region[:, :, None] == region[:, None, :]) & (open_key[:, None, :] | diagonal[None])
    scores = jnp.where(allowed[:, None], scores, jnp.float32(-1e+30))
    peak_score = lax.optimization_barrier(jnp.max(scores, axis=-1, keepdims=True))
    exp_scores = jnp.exp(scores - peak_score)
    weights = (exp_scores / lax.optimization_barrier(jnp.sum(exp_scores, axis=-1, keepdims=True))).astype(jnp.bfloat16)
    context = jnp.einsum('whqk,wkhd->wqhd', weights.astype(jnp.float32), value_heads.astype(jnp.float32))
    context = context.astype(jnp.bfloat16).reshape(-1, local_width)
    return jnp.dot(context, w_proj, preferred_element_type=jnp.float32).reshape(north_south_circles, columns, levels, features)

def level_decoder(latent, level_query, w_dec_q, w_dec_kv, w_dec_o):
    north_south_circles, columns, levels, features = latent.shape
    local_width = w_dec_kv.shape[2]
    head_count = local_width // HD
    patches = north_south_circles * columns
    normed = layer_norm(latent.astype(jnp.float32)).astype(jnp.bfloat16).reshape(-1, features)
    dkeys = jnp.dot(normed, w_dec_kv[0], preferred_element_type=jnp.float32).astype(jnp.bfloat16)
    dvals = jnp.dot(normed, w_dec_kv[1], preferred_element_type=jnp.float32).astype(jnp.bfloat16)
    dkeys = dkeys.reshape(patches, levels, head_count, HD)
    dvals = dvals.reshape(patches, levels, head_count, HD)
    dquery = jnp.dot(level_query, w_dec_q, preferred_element_type=jnp.float32).reshape(-1, head_count, HD)
    scores = jnp.einsum('lhd,pjhd->plhj', dquery, dkeys.astype(jnp.float32)) * HD ** (-0.5)
    peak_score = lax.optimization_barrier(jnp.max(scores, axis=-1, keepdims=True))
    exp_scores = jnp.exp(scores - peak_score)
    dweights = (exp_scores / lax.optimization_barrier(jnp.sum(exp_scores, axis=-1, keepdims=True))).astype(jnp.bfloat16)
    dcontext = jnp.einsum('plhj,pjhd->plhd', dweights.astype(jnp.float32), dvals.astype(jnp.float32))
    dcontext = dcontext.astype(jnp.bfloat16).reshape(-1, local_width)
    return jnp.dot(dcontext, w_dec_o, preferred_element_type=jnp.float32)

def reference(tokens, key_mask, w_qkv, w_proj, w_up, w_down, level_query, w_dec_q, w_dec_kv, w_dec_o, decode_matrix):
    north_south_circles, east_west_bands_set, levels, features = tokens.shape
    half_lat = WIN_LAT // 2
    half_lon = WINDOW_EASTWARD // 2
    block_count = east_west_bands_set // WINDOW_EASTWARD
    rolled = jnp.roll(tokens, (-half_lat, -half_lon), (0, 1))
    rolled_mask = jnp.roll(key_mask, (-half_lat, -half_lon), (0, 1))
    rolled = jnp.moveaxis(rolled.reshape(north_south_circles, block_count, WINDOW_EASTWARD, levels, features), 1, 0)
    rolled_mask = jnp.moveaxis(rolled_mask.reshape(north_south_circles, block_count, WINDOW_EASTWARD), 1, 0)

    def attend(block_pair):
        return window_attention(block_pair[0], block_pair[1], 0, north_south_circles, w_qkv, w_proj)
    attended = lax.map(attend, (rolled, rolled_mask))
    attended = jnp.moveaxis(attended, 0, 1).reshape(north_south_circles, east_west_bands_set, levels, features)
    attended = jnp.roll(attended, (half_lat, half_lon), (0, 1))
    x_one = tokens.astype(jnp.float32) + attended
    x_blocks = jnp.moveaxis(x_one.reshape(north_south_circles, block_count, WINDOW_EASTWARD, levels, features), 1, 0)

    def finish(x_block):
        normed = layer_norm(x_block).astype(jnp.bfloat16)
        hidden = jax.nn.gelu(jnp.dot(normed, w_up, preferred_element_type=jnp.float32), approximate=False).astype(jnp.bfloat16)
        latent = (x_block + jnp.dot(hidden, w_down, preferred_element_type=jnp.float32)).astype(jnp.bfloat16)
        dec_hidden = level_decoder(latent, level_query, w_dec_q, w_dec_kv, w_dec_o)
        cell_measures = jnp.dot(dec_hidden, decode_matrix, precision=lax.Precision.HIGHEST, preferred_element_type=jnp.float32)
        return cell_measures.reshape(north_south_circles, WINDOW_EASTWARD, ISOBAR_NUMBER, TARGET_QUANTITY, SQUARE_SPAN, SQUARE_SPAN)
    cell_measures = lax.map(finish, x_blocks)
    estimated_maps = jnp.transpose(cell_measures, (4, 3, 1, 5, 0, 2, 6))
    return estimated_maps.reshape(TARGET_QUANTITY, ISOBAR_NUMBER, north_south_circles * SQUARE_SPAN, east_west_bands_set * SQUARE_SPAN)
```

```python
import functools

import jax
import jax.numpy as jnp
import numpy as np
from jax import lax
from jax.experimental import pallas as pl
from jax.experimental.pallas import tpu as pltpu
from jax.sharding import PartitionSpec as P

HD = 64
ISOBAR_NUMBER = 13
SQUARE_SPAN = 4
WIN_LAT = 6
HALF_LAT = WIN_LAT // 2
LEVEL_LANES = 16
EPSILON = 1e-05
MASKED = -1e30
LOG2E = 1.4426950408889634
F32 = jnp.float32
BF16 = jnp.bfloat16

LOGIT_EDGE = 42.25
LOGIT_FIT = (
    -2.3022119998931885,
    -0.10482488572597504,
    8.28855627332814e-05,
    0.0001645075244596228,
    -1.2458292985684238e-05,
    4.844653744839889e-07,
    -9.89482717983492e-09,
    8.271171941798272e-11,
)

NT = (((1,), (1,)), ((), ()))


def from_behind(shard, axis, by):
    peers = lax.axis_size(axis)
    return lax.ppermute(shard, axis, [(i, (i + by) % peers) for i in range(peers)])


def mm(left, right):
    return jnp.dot(left, right, preferred_element_type=F32)


def layer_norm(values):
    center = values - jnp.mean(values, axis=-1, keepdims=True)
    spread = jnp.mean(center * center, axis=-1, keepdims=True)
    return center * lax.rsqrt(spread + EPSILON)


def gelu(x):
    square = jnp.minimum(x * x, LOGIT_EDGE)
    fit = jnp.full_like(x, LOGIT_FIT[-1])
    for coefficient in LOGIT_FIT[-2::-1]:
        fit = fit * square + coefficient
    return x / (1.0 + jnp.exp2(x * fit))


def split_bf16(values, terms):
    parts = []
    for _ in range(terms):
        part = values.astype(BF16)
        parts.append(part)
        values = values - part.astype(F32)
    return parts


def call(body, out_shape, scratch=(), flops=0):
    return pl.pallas_call(
        body,
        out_shape=out_shape,
        scratch_shapes=list(scratch),
        cost_estimate=pl.CostEstimate(flops=flops, transcendentals=0, bytes_accessed=1 << 20),
        compiler_params=pltpu.CompilerParams(vmem_limit_bytes=56 * 2**20),
    )


def select_body(total_rows, own_rows, first, tokens, place, out):
    halves = out.shape[0] // (tokens.shape[1] * own_rows)
    start = lax.axis_index("var") * own_rows
    source = place[:, 0:1] + start
    source = jnp.where(source >= total_rows, source - total_rows, source) + place[:, 1:2]
    column = lax.broadcasted_iota(jnp.int32, (2 * own_rows, 2 * total_rows), 1)
    chooser = (column == source).astype(F32).astype(BF16)
    for level in range(tokens.shape[1]):
        for c in range(0, halves, 2):
            pair = jnp.concatenate([tokens[first + c, level], tokens[first + c + 1, level]], axis=0)
            base = (level * halves + c) * own_rows
            out[base : base + 2 * own_rows, :] = mm(chooser, pair).astype(BF16)


def decoder_weights_body(w_q, w_kv, w_o, query, unembed, scores_out, values_out):
    heads = w_q.shape[1] // HD
    width = heads * HD
    mixed = jnp.zeros((width, width), F32)
    for part in split_bf16(unembed[...], 3):
        mixed += lax.dot_general(w_o[...], part, NT, preferred_element_type=F32)
    row = lax.broadcasted_iota(jnp.int32, (width, width), 0) // HD
    col = lax.broadcasted_iota(jnp.int32, (width, width), 1) // HD
    mixed = jnp.where(row == col, mixed, 0.0)
    values = jnp.zeros((w_kv.shape[1], width), F32)
    for part in split_bf16(mixed, 3):
        values += mm(w_kv[1], part)
    values_out[...] = values.astype(BF16)
    dquery = lax.dot_general(w_q[...], query[...], (((0,), (1,)), ((), ())), preferred_element_type=F32)
    row = lax.broadcasted_iota(jnp.int32, dquery.shape, 0) // HD
    col = lax.broadcasted_iota(jnp.int32, dquery.shape, 1) // LEVEL_LANES
    dquery = jnp.where(row == col, dquery * (LOG2E * HD ** (-0.5)), 0.0)
    scores = jnp.zeros((w_kv.shape[1], dquery.shape[1]), F32)
    for part in split_bf16(dquery, 3):
        scores += mm(w_kv[0], part)
    high, low = split_bf16(scores, 2)
    scores_out[...] = jnp.concatenate([high, low], axis=1)


def attention_body(
    windows, own, far, key_bias, side_q, side_k, wqkv_a, wqkv_b, wproj_a, wproj_b, out, normed, qkv, context
):
    levels = 3
    block = own.shape[0] // levels
    tokens = normed.shape[0]
    pairs = qkv.shape[0] // 3
    win_tokens = tokens // windows
    halves = (own, far)
    for level in range(levels):
        for side in range(2):
            base = (level * 2 + side) * block
            x = halves[side][level * block : (level + 1) * block, :].astype(F32)
            normed[base : base + block, :] = layer_norm(x).astype(BF16)
    for which in range(3):
        for side, weight in enumerate((wqkv_a, wqkv_b)):
            result = mm(normed[...], weight[which])
            for i in range(pairs // 2):
                qkv[which * pairs + side * (pairs // 2) + i] = result[:, i * 128 : (i + 1) * 128]
    lane = lax.broadcasted_iota(jnp.int32, (win_tokens, 2 * HD), 1)
    diagonal = lax.broadcasted_iota(jnp.int32, (win_tokens, win_tokens), 0) == lax.broadcasted_iota(
        jnp.int32, (win_tokens, win_tokens), 1
    )
    is_last_core = lax.axis_index("var") == lax.axis_size("var") - 1
    ones = jnp.ones((win_tokens, 2 * HD), BF16)

    def one_window(w, carry):
        rows = pl.ds(w, win_tokens, stride=windows)
        cross = jnp.where(jnp.logical_and(is_last_core, w == windows - 1), MASKED, 0.0)
        bias = jnp.where(side_q[...] != side_k[...], cross, 0.0)
        bias = jnp.where(diagonal, 0.0, jnp.minimum(bias, key_bias[w]))
        for t in range(pairs):
            q = qkv[t, rows, :]
            k = qkv[pairs + t, rows, :].astype(BF16)
            v = jnp.concatenate([qkv[2 * pairs + t, rows, :].astype(BF16), ones], axis=1)
            parts = []
            for head in range(2):
                mine = lane < HD if head == 0 else lane >= HD
                scores = lax.dot_general(
                    jnp.where(mine, q, 0.0).astype(BF16), k, NT, preferred_element_type=F32
                )
                scores = scores + bias
                peak = jnp.max(scores, axis=-1, keepdims=True)
                weights = jnp.exp2((scores - peak) * (LOG2E * HD ** (-0.5)))
                mixed = mm(weights.astype(BF16), v)
                parts.append(mixed[:, : 2 * HD] / mixed[:, 2 * HD :])
            context[t, rows, :] = jnp.where(lane < HD, parts[0], parts[1])
        return carry

    lax.fori_loop(0, windows, one_window, 0)
    attended = jnp.zeros((tokens, out.shape[1]), F32)
    for side, weight in enumerate((wproj_a, wproj_b)):
        both = [context[side * (pairs // 2) + i] for i in range(pairs // 2)]
        attended += mm(jnp.concatenate(both, axis=1).astype(BF16), weight[...])
    for level in range(levels):
        for side in range(2):
            base = (level * 2 + side) * block
            x = halves[side][level * block : (level + 1) * block, :].astype(F32)
            out[base : base + block, :] = x + attended[base : base + block]


def tail_body(
    own_rows,
    x_one,
    wup_a,
    wup_b,
    wdown_a,
    wdown_b,
    values_a,
    values_b,
    scores_a,
    scores_b,
    column_source,
    row_source,
    keep,
    send,
    mixed,
    scores,
    stacked,
):
    levels, patches, width = mixed.shape
    half = width // 2
    step = 512

    def one_level(level, carry):
        rows = pl.ds(pl.multiple_of(level * patches, 8), patches)
        x = x_one[rows, :]
        normed = layer_norm(x).astype(BF16)
        total = x
        for up, down in ((wup_a, wdown_a), (wup_b, wdown_b)):
            for k in range(0, up.shape[1], step):
                hidden = gelu(mm(normed, up[:, k : k + step])).astype(BF16)
                total = total + mm(hidden, down[k : k + step, :])
        latent = total.astype(BF16).astype(F32)
        normed = layer_norm(latent).astype(BF16)
        mixed[level, :, :half] = mm(normed, values_a[...])
        mixed[level, :, half:] = mm(normed, values_b[...])
        first = mm(normed, scores_a[...])
        second = mm(normed, scores_b[...])
        lane = lax.broadcasted_iota(jnp.int32, first.shape, 1)
        high = jnp.where(lane < HD, first, pltpu.roll(second, HD, 1))
        low = jnp.where(lane < HD, pltpu.roll(first, HD, 1), second)
        scores[level] = high + low
        return carry

    lax.fori_loop(0, levels, one_level, 0)
    peak = jnp.maximum(jnp.maximum(scores[0], scores[1]), scores[2])
    exps = [jnp.exp2(scores[level] - peak) for level in range(levels)]
    share = 1.0 / (exps[0] + exps[1] + exps[2])
    weight_0 = (exps[0] * share).astype(BF16)
    weight_1 = (exps[1] * share).astype(BF16)
    mixed[0] = mixed[0] - mixed[2]
    mixed[1] = mixed[1] - mixed[2]
    spread = lax.broadcasted_iota(jnp.int32, (2 * HD, width), 0) - LEVEL_LANES * (
        lax.broadcasted_iota(jnp.int32, (2 * HD, width), 1) // HD
    )
    low_lanes = lax.broadcasted_iota(jnp.int32, (own_rows, 2 * HD), 1) < HD

    def one_isobar(isobar, carry):
        expand = (spread == isobar).astype(F32).astype(BF16)
        pixels = mixed[2] + mm(weight_0, expand) * mixed[0] + mm(weight_1, expand) * mixed[1]
        folded = pixels[:, :128]
        for tile in range(1, width // 128):
            folded = folded + pixels[:, tile * 128 : (tile + 1) * 128]
        folded = folded + pltpu.roll(folded, HD, 1)
        rows = pl.ds(pl.multiple_of(isobar * own_rows, 8), own_rows)
        for pair in range(patches // own_rows // 2):
            even = folded[(2 * pair) * own_rows : (2 * pair + 1) * own_rows]
            odd = folded[(2 * pair + 1) * own_rows : (2 * pair + 2) * own_rows]
            stacked[rows, pair * 128 : (pair + 1) * 128] = jnp.where(low_lanes, even, odd)
        return carry

    lax.fori_loop(0, ISOBAR_NUMBER, one_isobar, 0)
    lanes = stacked.shape[1]
    by_column = lax.broadcasted_iota(jnp.int32, (lanes, lanes), 0) == column_source[...]
    result = mm(stacked[...].astype(BF16), by_column.astype(F32).astype(BF16)).astype(BF16)
    by_row = (
        lax.broadcasted_iota(jnp.int32, (row_source.shape[0], stacked.shape[0]), 1) == row_source[...]
    )
    result = mm(by_row.astype(F32).astype(BF16), result).astype(BF16)
    keep[...] = result[:, : lanes // 2]
    send[...] = result[:, lanes // 2 :]


def assemble_body(shift, pieces, row_source, out):
    sources, piece_rows, lanes = pieces.shape
    per_source = lanes // (out.shape[0] * SQUARE_SPAN)
    band_rows = out.shape[2]
    by_row = lax.broadcasted_iota(
        jnp.int32, (row_source.shape[0], SQUARE_SPAN * piece_rows), 1
    ) == row_source[...]
    by_row = by_row.astype(F32).astype(BF16)
    for v in range(out.shape[0]):
        stack = []
        for a in range(SQUARE_SPAN):
            at = (v * SQUARE_SPAN + a) * per_source
            stack.append(
                jnp.concatenate([pieces[g, :, at : at + per_source] for g in range(sources)], axis=1)
            )
        image = mm(by_row, jnp.concatenate(stack, axis=0))
        image = pltpu.roll(image, shift, 1)
        out[v] = image.reshape(ISOBAR_NUMBER, band_rows, image.shape[1])


def local(
    tokens,
    key_mask,
    w_qkv,
    w_proj,
    w_up,
    w_down,
    level_query,
    w_dec_q,
    w_dec_kv,
    w_dec_o,
    decode_matrix,
):
    total_rows, columns, levels, features = tokens.shape
    cores = lax.axis_size("var")
    core = lax.axis_index("var")
    peers = lax.axis_size("grid")
    half_cols = columns // 2
    own_rows = total_rows // cores
    windows = own_rows // WIN_LAT
    patches = columns * own_rows
    token_count = patches * levels
    outputs = decode_matrix.shape[1]
    variables = outputs // SQUARE_SPAN**2
    own_variables = variables // cores
    local_heads = w_dec_q.shape[1] // HD
    row_start = core * own_rows

    by_column = jnp.transpose(tokens, (1, 2, 0, 3))
    r6, w4 = np.meshgrid(np.arange(WIN_LAT), np.arange(windows), indexing="ij")
    place = (w4 * WIN_LAT + r6 + HALF_LAT).reshape(-1)
    place = np.stack(
        [np.concatenate([place, place]), np.repeat([0, total_rows], own_rows)], axis=1
    ).astype(np.int32)
    half_shape = jax.ShapeDtypeStruct((levels * half_cols * own_rows, features), BF16)

    def select(first):
        body = functools.partial(select_body, total_rows, own_rows, first)
        return call(body, half_shape)(by_column, place)

    west = select(0)
    far = from_behind(west, "grid", -1)

    open_marks = key_mask.astype(BF16)
    marks_right = from_behind(open_marks[:, :half_cols], "grid", -1)
    wqkv_far = from_behind(w_qkv, "var", 1)
    wproj_far = from_behind(w_proj, "var", 1)
    wup_far = from_behind(w_up, "var", 1)
    wdown_far = from_behind(w_down, "var", 1)

    own = select(half_cols)
    query = jnp.pad(level_query, ((0, LEVEL_LANES - ISOBAR_NUMBER), (0, 0)))
    query = jnp.tile(query, (local_heads, 1))
    unembed = jnp.tile(decode_matrix.T, (local_heads, 1))
    scores_w, values_w = call(
        decoder_weights_body,
        (
            jax.ShapeDtypeStruct((features, 2 * local_heads * LEVEL_LANES), BF16),
            jax.ShapeDtypeStruct((features, local_heads * HD), BF16),
        ),
    )(w_dec_q, w_dec_kv, w_dec_o, query, unembed)
    scores_far = from_behind(scores_w, "var", 1)
    values_far = from_behind(values_w, "var", 1)

    marks = jnp.concatenate([open_marks[:, half_cols:], marks_right], axis=1)
    marks = jnp.roll(marks, -HALF_LAT, 0)
    marks = lax.dynamic_slice_in_dim(marks, row_start, own_rows, 0)
    key_bias = jnp.where(marks > 0, 0.0, MASKED).astype(F32)
    key_bias = jnp.transpose(key_bias.reshape(windows, WIN_LAT, columns), (0, 2, 1))
    key_bias = jnp.tile(key_bias.reshape(windows, 1, columns * WIN_LAT), (1, 1, levels))
    side = np.tile((np.arange(WIN_LAT) >= HALF_LAT).astype(np.float32), levels * columns)
    pairs = 2 * local_heads // 2
    x_one = call(
        functools.partial(attention_body, windows),
        jax.ShapeDtypeStruct((token_count, features), F32),
        scratch=[
            pltpu.VMEM((token_count, features), BF16),
            pltpu.VMEM((3 * pairs, token_count, 2 * HD), F32),
            pltpu.VMEM((pairs, token_count, 2 * HD), F32),
        ],
        flops=2 * 10**9,
    )(own, far, key_bias, side[:, None], side[None, :], w_qkv, wqkv_far, w_proj, wproj_far)

    lanes = columns * outputs
    index = np.arange(lanes)
    per_core = lanes // cores
    which, rest = index // per_core, index % per_core
    v, rest = rest // (per_core // own_variables), rest % (per_core // own_variables)
    a, rest = rest // (columns * SQUARE_SPAN), rest % (columns * SQUARE_SPAN)
    c, b = rest // SQUARE_SPAN, rest % SQUARE_SPAN
    column_source = (c * outputs + (v * SQUARE_SPAN + a) * SQUARE_SPAN + b)[None, :].astype(np.int32)
    which = which[None, :].astype(np.int32)
    column_source = column_source + (outputs // cores) * ((which + core) % cores)
    blocks = own_rows // HALF_LAT
    block_rows = -(-ISOBAR_NUMBER * HALF_LAT // 8) * 8
    row_source = np.full((blocks, block_rows), -1, np.int32)
    i, isobar, r = np.meshgrid(
        np.arange(blocks), np.arange(ISOBAR_NUMBER), np.arange(HALF_LAT), indexing="ij"
    )
    source = isobar * own_rows + ((i % 2) * HALF_LAT + r) * windows + i // 2
    row_source[:, : ISOBAR_NUMBER * HALF_LAT] = source.reshape(blocks, -1)
    block_shape = jax.ShapeDtypeStruct((blocks * block_rows, per_core), BF16)
    keep, send = call(
        functools.partial(tail_body, own_rows),
        (block_shape, block_shape),
        scratch=[
            pltpu.VMEM((levels, patches, 2 * local_heads * HD), F32),
            pltpu.VMEM((levels, patches, 2 * local_heads * LEVEL_LANES), F32),
            pltpu.VMEM((ISOBAR_NUMBER * own_rows, lanes), F32),
        ],
        flops=6 * 10**9,
    )(
        x_one,
        w_up,
        wup_far,
        w_down,
        wdown_far,
        values_w,
        values_far,
        scores_w,
        scores_far,
        column_source,
        row_source.reshape(-1, 1),
    )
    got = from_behind(send, "var", 1)
    keep = keep.reshape(blocks, block_rows, per_core)
    got = got.reshape(blocks, block_rows, per_core)
    every = jnp.where(core == 0, jnp.concatenate([keep, got]), jnp.concatenate([got, keep]))
    every = jnp.roll(every, 1, 0)
    pixel_rows = total_rows * SQUARE_SPAN // peers
    shift = half_cols * SQUARE_SPAN
    out_shape = (own_variables, ISOBAR_NUMBER, pixel_rows, peers * columns * SQUARE_SPAN)
    if pixel_rows == WIN_LAT * SQUARE_SPAN:
        pieces = lax.all_to_all(
            every.reshape(peers, 2 * block_rows, per_core), "grid", split_axis=0, concat_axis=0, tiled=True
        )
        isobar, r, a = np.meshgrid(
            np.arange(ISOBAR_NUMBER), np.arange(WIN_LAT), np.arange(SQUARE_SPAN), indexing="ij"
        )
        source = a * 2 * block_rows + (r // HALF_LAT) * block_rows + isobar * HALF_LAT + r % HALF_LAT
        return call(
            functools.partial(assemble_body, shift),
            jax.ShapeDtypeStruct(out_shape, F32),
        )(pieces, source.reshape(-1, 1).astype(np.int32))
    every = every[:, : ISOBAR_NUMBER * HALF_LAT].reshape(
        2 * blocks, ISOBAR_NUMBER, HALF_LAT, own_variables, SQUARE_SPAN, columns * SQUARE_SPAN
    )
    every = jnp.transpose(every, (3, 1, 0, 2, 4, 5)).reshape(
        own_variables, ISOBAR_NUMBER, total_rows * SQUARE_SPAN, columns * SQUARE_SPAN
    )
    image = lax.all_to_all(every, "grid", split_axis=2, concat_axis=3, tiled=True)
    return jnp.roll(image, shift, 3).astype(F32)


def solution(mesh):
    placed = (
        P("group", "grid", None, None),
        P("group", "grid"),
        P(None, None, "var"),
        P("var", None),
        P(None, "var"),
        P("var", None),
        P(),
        P(None, "var"),
        P(None, None, "var"),
        P("var", None),
        P(),
    )
    return jax.shard_map(
        local,
        mesh=mesh,
        in_specs=placed,
        out_specs=P("var", "group", "grid", None),
        check_vma=False,
    )
```
